32 devices in a mesh: tp: 4 (over x, core), grp: 8 (over z, y).
Axes of the slice: x: 2, y: 2, z: 4, core: 2. Of those that a mesh axis runs over, the one named last changes fastest.
Arguments:
- flat_shards: bfloat16 [2, 2, 8256, 24576], P(None, None, ('grp', 'tp')), may hold values from -0.0625 to 0.0625
- offsets: int32 [2, 2], replicated, may hold values from 0 to 2
- probes: bfloat16 [512, 8192], P(None, 'grp'), may hold values from -6 to 6
Outputs:
- serving_tiles: bfloat16 [2, 2, 8192, 24576], P(None, None, 'grp', 'tp')
- hidden_check: bfloat16 [2, 512, 24576], P(None, 'grp', 'tp')
The draws below stay inside these ranges and needn't reach their ends.
All inputs are finite; a program needn't handle non-finite values.
Results may differ from the reference program's by a relative error of at most 0.001.
Values may be sent and summed in bfloat16 or wider, within the bound.
A program may use at most 320 MiB of HBM per device.

```python
import jax
import jax.numpy as jnp
from jax import lax

D = 8192
FF = 24576
LAYERS = 2
PAD = 2
PROBES = 512
ROWS_DEV = 256
N_GRP = 8
DEVICES = 32


def place_ends(result, rng, least, largest):
    longest = result.shape.index(max(result.shape))
    spots = []
    for shift in (0, 1):
        where = [jax.random.randint(jax.random.fold_in(rng, axis), (), 0, length) for axis, length in enumerate(result.shape)]
        where[longest] = (where[longest] + shift) % result.shape[longest]
        spots.append(tuple(where))
    return result.at[spots[0]].set(least).at[spots[1]].set(largest)


def level_of(key, extent, cuts, low, high):
    loudness, own = 1.0, jax.random.fold_in(key, 6)
    for axis_at, blocks in cuts:
        heights = jnp.exp(jax.random.uniform(jax.random.fold_in(own, axis_at), (blocks,), jnp.float32, low / len(cuts), high / len(cuts)))
        loudness = loudness * jnp.repeat(heights, extent[axis_at] // blocks).reshape([-1 if axis == axis_at else 1 for axis in range(len(extent))])
    return loudness


def bell_draw(key, shape, width, most, split=(), dtype=jnp.bfloat16):
    entries = jax.random.normal(key, shape, jnp.float32) * width
    if len(split) > 0:
        entries = level_of(key, shape, split, -0.22, 0.18) * entries
    return jnp.clip(entries, min=-most, max=most).astype(dtype)


def setup_inputs(seed: int = 0) -> dict:
    arg_keys = jax.random.split(jax.random.key(seed), 4)
    flat_shards = bell_draw(arg_keys[0], (LAYERS, 2, DEVICES * (ROWS_DEV + PAD), FF), D ** -0.5, 0.0625, ((2, 32),))
    offsets = place_ends(jax.random.randint(arg_keys[1], (LAYERS, 2), 0, PAD + 1), jax.random.fold_in(arg_keys[1], 1), 0, PAD).astype(jnp.int32)
    probes = bell_draw(arg_keys[2], (PROBES, D), 1.0, 6.0, ((1, 8),))
    return {"flat_shards": flat_shards, "offsets": offsets, "probes": probes}


def checksum(probes, tile):
    block = D // N_GRP

    def add_block(index, total):
        start = (index * block).astype(jnp.int32)
        rows = lax.dynamic_slice_in_dim(probes, start, block, 1)
        part = lax.dynamic_slice_in_dim(tile, start, block, 0)
        term = jnp.dot(rows, part, preferred_element_type=jnp.float32)
        return total + term

    empty = jnp.zeros((probes.shape[0], tile.shape[1]), jnp.float32)
    return lax.fori_loop(jnp.int32(0), jnp.int32(N_GRP), add_block, empty)


def reference(flat_shards, offsets, probes):
    layer_list = []
    check_list = []
    for which_layer in range(LAYERS):
        tensor_list = []
        for which_tensor in range(2):
            blocks = flat_shards[which_layer, which_tensor].reshape(DEVICES, ROWS_DEV + PAD, FF)
            start = offsets[which_layer, which_tensor].astype(jnp.int32)
            picked = lax.dynamic_slice_in_dim(blocks, start, ROWS_DEV, 1)
            tensor_list.append(picked.reshape(D, FF))
        gate_sums = checksum(probes, tensor_list[0])
        up_sums = checksum(probes, tensor_list[1])
        check_list.append((jax.nn.silu(gate_sums) * up_sums).astype(jnp.bfloat16))
        layer_list.append(jnp.stack(tensor_list))
    return jnp.stack(layer_list), jnp.stack(check_list)
```

```python
import functools

import jax
import jax.numpy as jnp
from jax import lax
from jax.experimental import pallas as pl
from jax.experimental.pallas import tpu as pltpu
from jax.sharding import PartitionSpec as P

PAD = 2
CHUNK = 512
SLOTS = 6
MESH = pl.DeviceIdType.MESH


def ring_device(place, count):
    half = count // 2
    back = lax.div(place, half)
    return (1 - back) * 2 * place + back * (2 * (count - 1 - place) + 1)


def exchange(
    tp_count,
    grp_count,
    flat_ref,
    tails_ref,
    main_ref,
    rest_ref,
    raw_ref,
    ends_ref,
    check_ref,
    xbuf,
    tailbuf,
    partial,
    outgoing,
    incoming,
    gate_sums,
    x_send,
    x_recv,
    x_free,
    own_sem,
    raw_sem,
    tail_send,
    tail_recv,
    tail_own,
    ends_sem,
    ring_send,
    ring_recv,
    ring_free,
):
    t = lax.axis_index("tp")
    g = lax.axis_index("grp")
    odd = lax.rem(g, 2)
    place = (1 - odd) * lax.div(g, 2) + odd * (grp_count - 1 - lax.div(g, 2))
    after = ring_device(lax.rem(place + 1, grp_count), grp_count)
    before = ring_device(lax.rem(place + grp_count - 1, grp_count), grp_count)
    toward = (after, before)
    origin = (before, after)

    pair_count = flat_ref.shape[0]
    rows = xbuf.shape[1] // tp_count
    columns = raw_ref.shape[2]
    chunk = xbuf.shape[2]
    per_layer = columns // chunk * 2
    total = columns // chunk * pair_count
    share = main_ref.shape[1] // grp_count
    half = share // 2
    hops = grp_count - 1

    def spot(index):
        layer = lax.div(index, per_layer)
        inside = lax.rem(index, per_layer)
        return layer * 2 + lax.rem(inside, 2), lax.div(inside, 2)

    def x_copy(index, step):
        pair, block = spot(index)
        slot = lax.rem(index, SLOTS)
        partner = lax.rem(t + step, tp_count)
        start = pl.multiple_of(partner * columns + block * chunk, chunk)
        return pltpu.make_async_remote_copy(
            src_ref=flat_ref.at[pair, pl.ds(0, rows), pl.ds(start, chunk)],
            dst_ref=xbuf.at[slot, pl.ds(pl.multiple_of(t * rows, rows), rows), :],
            send_sem=x_send.at[step - 1, slot],
            recv_sem=x_recv.at[step - 1, slot],
            device_id=(partner, g),
            device_id_type=MESH,
        )

    def x_arrival(index, step):
        slot = lax.rem(index, SLOTS)
        source = lax.rem(t + tp_count - step, tp_count)
        landing = xbuf.at[slot, pl.ds(pl.multiple_of(source * rows, rows), rows), :]
        return pltpu.make_async_remote_copy(
            src_ref=landing,
            dst_ref=landing,
            send_sem=x_send.at[step - 1, slot],
            recv_sem=x_recv.at[step - 1, slot],
            device_id=(source, g),
            device_id_type=MESH,
        )

    def own_copy(index):
        pair, block = spot(index)
        slot = lax.rem(index, SLOTS)
        start = pl.multiple_of(t * columns + block * chunk, chunk)
        return pltpu.make_async_copy(
            flat_ref.at[pair, pl.ds(0, rows), pl.ds(start, chunk)],
            xbuf.at[slot, pl.ds(pl.multiple_of(t * rows, rows), rows), :],
            own_sem.at[slot],
        )

    def raw_copy(index):
        pair, block = spot(index)
        slot = lax.rem(index, SLOTS)
        return pltpu.make_async_copy(
            xbuf.at[slot],
            raw_ref.at[pair, :, pl.ds(pl.multiple_of(block * chunk, chunk), chunk)],
            raw_sem.at[slot],
        )

    def tail_copy(step):
        partner = lax.rem(t + step, tp_count)
        return pltpu.make_async_remote_copy(
            src_ref=tails_ref.at[:, pl.ds(pl.multiple_of(partner * columns, chunk), columns)],
            dst_ref=tailbuf.at[t],
            send_sem=tail_send.at[step - 1],
            recv_sem=tail_recv.at[step - 1],
            device_id=(partner, g),
            device_id_type=MESH,
        )

    def tail_arrival(step):
        source = lax.rem(t + tp_count - step, tp_count)
        return pltpu.make_async_remote_copy(
            src_ref=tailbuf.at[source],
            dst_ref=tailbuf.at[source],
            send_sem=tail_send.at[step - 1],
            recv_sem=tail_recv.at[step - 1],
            device_id=(source, g),
            device_id_type=MESH,
        )

    def ring_copy(way, stage, turn):
        return pltpu.make_async_remote_copy(
            src_ref=outgoing.at[way, stage, turn],
            dst_ref=incoming.at[way, stage, turn],
            send_sem=ring_send.at[way, stage, turn],
            recv_sem=ring_recv.at[way, stage, turn],
            device_id=(t, toward[way]),
            device_id_type=MESH,
        )

    def own_rows(way, stage):
        if way == 0:
            owner = lax.rem(place + 2 * grp_count - 1 - stage, grp_count)
        else:
            owner = lax.rem(place + 1 + stage, grp_count)
        first = ring_device(owner, grp_count) * share + way * half
        return pl.ds(pl.multiple_of(first, half), half)

    barrier = pltpu.get_barrier_semaphore()
    for step in range(1, tp_count):
        pl.semaphore_signal(
            barrier, inc=1, device_id=(lax.rem(t + step, tp_count), g), device_id_type=MESH
        )
    for way in range(2):
        pl.semaphore_signal(barrier, inc=1, device_id=(t, toward[way]), device_id_type=MESH)
    pl.semaphore_wait(barrier, tp_count - 1 + 2)

    for step in range(1, tp_count):
        tail_copy(step).start()
    own_tail = pltpu.make_async_copy(
        tails_ref.at[:, pl.ds(pl.multiple_of(t * columns, chunk), columns)],
        tailbuf.at[t],
        tail_own,
    )
    own_tail.start()

    @pl.loop(0, SLOTS - 1)
    def _(index):
        for step in range(1, tp_count):
            x_copy(index, step).start()
        own_copy(index).start()

    own_tail.wait()
    for step in range(1, tp_count):
        tail_arrival(step).wait_recv()
    ends = pltpu.make_async_copy(tailbuf, ends_ref, ends_sem)
    ends.start()

    @pl.loop(0, total + hops)
    def _(tick):
        turn = lax.rem(tick, 2)
        last_turn = 1 - turn

        @pl.when(jnp.logical_and(tick >= 2, tick < total + hops - 1))
        def _():
            for way in range(2):
                pl.semaphore_wait(ring_free.at[way], 1)

        for stage in range(hops, 0, -1):
            index = tick - stage

            @pl.when(jnp.logical_and(index >= 0, index < total))
            def _():
                place_of = lax.rem(index, grp_count)
                if stage < hops:

                    @pl.when(index >= 2)
                    def _():
                        for way in range(2):
                            ring_copy(way, stage, turn).wait_send()

                    for way in range(2):
                        ring_copy(way, stage - 1, last_turn).wait_recv()
                        outgoing[way, stage, turn] = (
                            incoming[way, stage - 1, last_turn]
                            + partial[place_of, own_rows(way, stage), :]
                        )
                        ring_copy(way, stage, turn).start()
                else:
                    pair, block = spot(index)
                    parts = []
                    for way in range(2):
                        ring_copy(way, stage - 1, last_turn).wait_recv()
                        parts.append(
                            incoming[way, stage - 1, last_turn]
                            + partial[place_of, own_rows(way, stage), :]
                        )
                    sums = jnp.concatenate(parts, axis=0)

                    @pl.when(lax.rem(pair, 2) == 0)
                    def _():
                        gate_sums[...] = sums

                    @pl.when(lax.rem(pair, 2) == 1)
                    def _():
                        gate = gate_sums[...]
                        hidden = gate / (1.0 + jnp.exp(-gate)) * sums
                        where = pl.ds(pl.multiple_of(block * chunk, chunk), chunk)
                        check_ref[lax.div(pair, 2), :, where] = hidden.astype(check_ref.dtype)

        @pl.when(tick < total)
        def _():
            slot = lax.rem(tick, SLOTS)
            kept = lax.rem(tick, grp_count)
            pair, block = spot(tick)
            own_copy(tick).wait()
            for step in range(1, tp_count):
                x_arrival(tick, step).wait_recv()
            raw_copy(tick).start()
            where = pl.ds(pl.multiple_of(block * chunk, chunk), chunk)
            tail = tailbuf[:, :, where].reshape(tp_count * tailbuf.shape[1], chunk)
            partial[kept] = jnp.dot(
                main_ref[pair], xbuf[slot], preferred_element_type=jnp.float32
            ) + jnp.dot(rest_ref[pair], tail, preferred_element_type=jnp.float32)

            @pl.when(tick >= 2)
            def _():
                for way in range(2):
                    ring_copy(way, 0, turn).wait_send()

            for way in range(2):
                outgoing[way, 0, turn] = partial[kept, own_rows(way, 0), :]
                ring_copy(way, 0, turn).start()

        @pl.when(jnp.logical_and(tick >= 1, tick < total + hops - 2))
        def _():
            for way in range(2):
                pl.semaphore_signal(
                    ring_free.at[way], inc=1, device_id=(t, origin[way]), device_id_type=MESH
                )

        @pl.when(jnp.logical_and(tick >= 1, tick < total + 1))
        def _():
            raw_copy(tick - 1).wait()

        ahead = tick + SLOTS - 1

        @pl.when(jnp.logical_and(tick >= 1, ahead < total))
        def _():
            for step in range(1, tp_count):
                pl.semaphore_signal(
                    x_free.at[step - 1],
                    inc=1,
                    device_id=(lax.rem(t + tp_count - step, tp_count), g),
                    device_id_type=MESH,
                )

        @pl.when(ahead < total)
        def _():
            @pl.when(tick >= 1)
            def _():
                for step in range(1, tp_count):
                    x_copy(ahead - SLOTS, step).wait_send()
                    pl.semaphore_wait(x_free.at[step - 1], 1)

            for step in range(1, tp_count):
                x_copy(ahead, step).start()
            own_copy(ahead).start()

    @pl.loop(total - SLOTS, total)
    def _(index):
        for step in range(1, tp_count):
            x_copy(index, step).wait_send()

    for stage in range(hops):
        for way in range(2):
            for turn in range(2):
                ring_copy(way, stage, turn).wait_send()
    for step in range(1, tp_count):
        tail_copy(step).wait_send()
    ends.wait()


def align(pair_tails, offsets_ref, raw_ref, ends_ref, tile_ref):
    pair = pl.program_id(0)
    start = offsets_ref[pair]
    rows, width = tile_ref.shape[1:]
    step = 256
    count = ends_ref.shape[1]

    @pl.when(start == 0)
    def _():
        tile_ref[...] = raw_ref[...]

    for shift in range(1, pair_tails + 1):

        @pl.when(start == shift)
        def _():
            @pl.loop(0, width // step)
            def _(at):
                where = pl.ds(pl.multiple_of(at * step, step), step)
                raw = raw_ref[0, :, where].astype(jnp.float32)
                ends = ends_ref[0, :, where].astype(jnp.float32)
                ends = pltpu.roll(ends, lax.rem(count - pair_tails * pair, count), 0)
                joined = jnp.concatenate([raw, ends], axis=0)
                tile_ref[0, :, where] = joined[shift : shift + rows].astype(tile_ref.dtype)


def per_device(flat_shards, offsets, probes):
    tp_count = lax.axis_size("tp")
    grp_count = lax.axis_size("grp")
    layers, tensors, shard, width = flat_shards.shape
    pairs = layers * tensors
    rows = shard - PAD
    columns = width // tp_count
    probe_count = probes.shape[0]
    chunk = CHUNK
    share = probe_count // grp_count
    half = share // 2
    hops = grp_count - 1

    starts = offsets.reshape(pairs)
    spread = jnp.pad(probes.reshape(probe_count, tp_count, rows), ((0, 0), (0, 0), (PAD, PAD)))
    shifts = [spread[:, :, PAD - shift : PAD - shift + shard] for shift in range(PAD + 1)]
    mains, rests = [], []
    for pair in range(pairs):
        moved = shifts[0]
        for shift in range(1, PAD + 1):
            moved = jnp.where(starts[pair] == shift, shifts[shift], moved)
        mains.append(moved[:, :, :rows].reshape(probe_count, tp_count * rows))
        sides = ((0, 0), (0, 0), (pair * PAD, (pairs - 1 - pair) * PAD))
        rests.append(jnp.pad(moved[:, :, rows:], sides).reshape(probe_count, tp_count * pairs * PAD))
    main, rest = jnp.stack(mains), jnp.stack(rests)
    flat = flat_shards.reshape(pairs, shard, width)
    tails = flat[:, rows:, :].reshape(pairs * PAD, width)

    anywhere = pl.BlockSpec(memory_space=pl.ANY)
    inside = pl.BlockSpec(memory_space=pltpu.VMEM)
    dma = pltpu.SemaphoreType.DMA
    regular = pltpu.SemaphoreType.REGULAR
    raw, ends, check = pl.pallas_call(
        functools.partial(exchange, tp_count, grp_count),
        out_shape=(
            jax.ShapeDtypeStruct((pairs, tp_count * rows, columns), flat.dtype),
            jax.ShapeDtypeStruct((tp_count, pairs * PAD, columns), flat.dtype),
            jax.ShapeDtypeStruct((layers, share, columns), jnp.bfloat16),
        ),
        in_specs=[anywhere, anywhere, inside, inside],
        out_specs=(anywhere, anywhere, inside),
        scratch_shapes=[
            pltpu.VMEM((SLOTS, tp_count * rows, chunk), flat.dtype),
            pltpu.VMEM((tp_count, pairs * PAD, columns), flat.dtype),
            pltpu.VMEM((grp_count, probe_count, chunk), jnp.float32),
            pltpu.VMEM((2, hops, 2, half, chunk), jnp.float32),
            pltpu.VMEM((2, hops, 2, half, chunk), jnp.float32),
            pltpu.VMEM((share, chunk), jnp.float32),
            dma((tp_count - 1, SLOTS)),
            dma((tp_count - 1, SLOTS)),
            regular((tp_count - 1,)),
            dma((SLOTS,)),
            dma((SLOTS,)),
            dma((tp_count - 1,)),
            dma((tp_count - 1,)),
            dma,
            dma,
            dma((2, hops, 2)),
            dma((2, hops, 2)),
            regular((2,)),
        ],
        compiler_params=pltpu.CompilerParams(
            collective_id=0, has_side_effects=True, vmem_limit_bytes=60 * 1024 * 1024
        ),
    )(flat, tails, main, rest)

    block = columns // 2
    tiles = pl.pallas_call(
        functools.partial(align, PAD),
        out_shape=jax.ShapeDtypeStruct((pairs, tp_count * rows, columns), flat.dtype),
        grid_spec=pltpu.PrefetchScalarGridSpec(
            num_scalar_prefetch=1,
            grid=(pairs, tp_count, columns // block),
            in_specs=[
                pl.BlockSpec((1, rows, block), lambda p, s, b, starts: (p, s, b)),
                pl.BlockSpec((1, pairs * PAD, block), lambda p, s, b, starts: (s, 0, b)),
            ],
            out_specs=pl.BlockSpec((1, rows, block), lambda p, s, b, starts: (p, s, b)),
        ),
    )(starts, raw, ends)
    return tiles.reshape(layers, tensors, tp_count * rows, columns), check


def solution(mesh):
    placed = (P(None, None, ("grp", "tp"), None), P(), P(None, "grp"))
    return jax.shard_map(
        per_device,
        mesh=mesh,
        in_specs=placed,
        out_specs=(P(None, None, "grp", "tp"), P(None, "grp", "tp")),
        check_vma=False,
    )
```

```python
import functools

import jax
import jax.numpy as jnp
from jax import lax
from jax.experimental import pallas as pl
from jax.experimental.pallas import tpu as pltpu
from jax.sharding import PartitionSpec as P

PAD = 2
WIDTH = 256
LANES = 128
SLOTS = 4
MESH = pl.DeviceIdType.MESH


def ring_device(place, count):
    half = count // 2
    back = lax.div(place, half)
    return (1 - back) * 2 * place + back * (2 * (count - 1 - place) + 1)


def exchange(
    tp_count,
    grp_count,
    flat_ref,
    offsets_ref,
    probes_ref,
    raw_ref,
    check_ref,
    inbuf,
    chosen,
    sending,
    xbuf,
    partial,
    outgoing,
    incoming,
    in_sem,
    x_send,
    x_recv,
    x_free,
    raw_sem,
    ring_send,
    ring_recv,
    ring_free,
):
    t = lax.axis_index("tp")
    g = lax.axis_index("grp")
    odd = lax.rem(g, 2)
    place = (1 - odd) * lax.div(g, 2) + odd * (grp_count - 1 - lax.div(g, 2))
    after = ring_device(lax.rem(place + 1, grp_count), grp_count)
    before = ring_device(lax.rem(place + grp_count - 1, grp_count), grp_count)
    toward = (after, before)
    origin = (before, after)

    layers, shard, tensors, _ = flat_ref.shape
    rows = shard - PAD
    columns = raw_ref.shape[3]
    chunk = xbuf.shape[2]
    width = chunk // tensors
    per_layer = columns // width
    total = layers * per_layer
    share = probes_ref.shape[0] // grp_count
    half = share // 2
    hops = grp_count - 1

    def fetch(index, step, piece):
        layer, block = lax.div(index, per_layer), lax.rem(index, per_layer)
        turn = lax.rem(index, 2)
        partner = lax.rem(t + step, tp_count)
        start = pl.multiple_of(partner * columns + block * width + piece * LANES, LANES)
        return pltpu.make_async_copy(
            flat_ref.at[layer, :, :, pl.ds(start, LANES)],
            inbuf.at[turn, step, piece],
            in_sem.at[turn, step, piece],
        )

    def fetch_all(index):
        for step in range(tp_count):
            for piece in range(width // LANES):
                fetch(index, step, piece).start()

    def choose(index):
        layer = lax.div(index, per_layer)
        turn, slot = lax.rem(index, 2), lax.rem(index, SLOTS)
        for step in list(range(1, tp_count)) + [0]:
            pieces = []
            for piece in range(width // LANES):
                fetch(index, step, piece).wait()
                pieces.append(inbuf[turn, step, piece].reshape(shard * tensors, LANES))
            both = jnp.concatenate(pieces, axis=1)
            for tensor in range(tensors):
                picked = jnp.dot(
                    chosen[layer * tensors + tensor], both, preferred_element_type=jnp.float32
                ).astype(xbuf.dtype)
                where = slice(tensor * width, (tensor + 1) * width)
                if step == 0:
                    xbuf[slot, pl.ds(pl.multiple_of(t * rows, rows), rows), where] = picked
                else:
                    sending[slot, step - 1, :, where] = picked

    def x_copy(index, step):
        slot = lax.rem(index, SLOTS)
        return pltpu.make_async_remote_copy(
            src_ref=sending.at[slot, step - 1],
            dst_ref=xbuf.at[slot, pl.ds(pl.multiple_of(t * rows, rows), rows), :],
            send_sem=x_send.at[step - 1, slot],
            recv_sem=x_recv.at[step - 1, slot],
            device_id=(lax.rem(t + step, tp_count), g),
            device_id_type=MESH,
        )

    def x_arrival(index, step):
        slot = lax.rem(index, SLOTS)
        source = lax.rem(t + tp_count - step, tp_count)
        landing = xbuf.at[slot, pl.ds(pl.multiple_of(source * rows, rows), rows), :]
        return pltpu.make_async_remote_copy(
            src_ref=landing,
            dst_ref=landing,
            send_sem=x_send.at[step - 1, slot],
            recv_sem=x_recv.at[step - 1, slot],
            device_id=(source, g),
            device_id_type=MESH,
        )

    def raw_copy(index, tensor):
        layer, block = lax.div(index, per_layer), lax.rem(index, per_layer)
        slot = lax.rem(index, SLOTS)
        where = pl.ds(pl.multiple_of(block * width, width), width)
        return pltpu.make_async_copy(
            xbuf.at[slot, :, pl.ds(tensor * width, width)],
            raw_ref.at[layer, tensor, :, where],
            raw_sem.at[slot, tensor],
        )

    def ring_copy(way, stage, turn):
        return pltpu.make_async_remote_copy(
            src_ref=outgoing.at[way, stage, turn],
            dst_ref=incoming.at[way, stage, turn],
            send_sem=ring_send.at[way, stage, turn],
            recv_sem=ring_recv.at[way, stage, turn],
            device_id=(t, toward[way]),
            device_id_type=MESH,
        )

    def own_rows(way, stage):
        if way == 0:
            owner = lax.rem(place + 2 * grp_count - 1 - stage, grp_count)
        else:
            owner = lax.rem(place + 1 + stage, grp_count)
        first = ring_device(owner, grp_count) * share + way * half
        return pl.ds(pl.multiple_of(first, half), half)

    fetch_all(0)
    fetch_all(1)
    at_row = lax.broadcasted_iota(jnp.int32, (rows, shard * tensors), 0)
    at_column = lax.broadcasted_iota(jnp.int32, (rows, shard * tensors), 1)
    for layer in range(layers):
        for tensor in range(tensors):
            wanted = (at_row + offsets_ref[layer, tensor]) * tensors + tensor
            chosen[layer * tensors + tensor] = jnp.where(at_column == wanted, 1.0, 0.0).astype(
                chosen.dtype
            )

    barrier = pltpu.get_barrier_semaphore()
    for step in range(1, tp_count):
        pl.semaphore_signal(
            barrier, inc=1, device_id=(lax.rem(t + step, tp_count), g), device_id_type=MESH
        )
    for way in range(2):
        pl.semaphore_signal(barrier, inc=1, device_id=(t, toward[way]), device_id_type=MESH)
    pl.semaphore_wait(barrier, tp_count - 1 + 2)

    @pl.loop(0, SLOTS - 1)
    def _(index):
        choose(index)
        for step in range(1, tp_count):
            x_copy(index, step).start()
        fetch_all(index + 2)

    @pl.loop(0, total + hops)
    def _(tick):
        turn = lax.rem(tick, 2)
        last_turn = 1 - turn

        @pl.when(jnp.logical_and(tick >= 2, tick < total + hops - 1))
        def _():
            for way in range(2):
                pl.semaphore_wait(ring_free.at[way], 1)

        for stage in range(hops, 0, -1):
            index = tick - stage

            @pl.when(jnp.logical_and(index >= 0, index < total))
            def _():
                place_of = lax.rem(index, grp_count)
                if stage < hops:

                    @pl.when(index >= 2)
                    def _():
                        for way in range(2):
                            ring_copy(way, stage, turn).wait_send()

                    for way in range(2):
                        ring_copy(way, stage - 1, last_turn).wait_recv()
                        outgoing[way, stage, turn] = (
                            incoming[way, stage - 1, last_turn]
                            + partial[place_of, own_rows(way, stage), :]
                        )
                        ring_copy(way, stage, turn).start()
                else:
                    layer, block = lax.div(index, per_layer), lax.rem(index, per_layer)
                    parts = []
                    for way in range(2):
                        ring_copy(way, stage - 1, last_turn).wait_recv()
                        parts.append(
                            incoming[way, stage - 1, last_turn]
                            + partial[place_of, own_rows(way, stage), :]
                        )
                    sums = jnp.concatenate(parts, axis=0)
                    gate, up = sums[:, :width], sums[:, width:]
                    hidden = gate / (1.0 + jnp.exp(-gate)) * up
                    where = pl.ds(pl.multiple_of(block * width, width), width)
                    check_ref[layer, :, where] = hidden.astype(check_ref.dtype)

        @pl.when(tick < total)
        def _():
            slot = lax.rem(tick, SLOTS)
            kept = lax.rem(tick, grp_count)
            for step in range(1, tp_count):
                x_arrival(tick, step).wait_recv()
            for tensor in range(tensors):
                raw_copy(tick, tensor).start()
            partial[kept] = jnp.dot(
                probes_ref[...], xbuf[slot], preferred_element_type=jnp.float32
            )

            @pl.when(tick >= 2)
            def _():
                for way in range(2):
                    ring_copy(way, 0, turn).wait_send()

            for way in range(2):
                outgoing[way, 0, turn] = partial[kept, own_rows(way, 0), :]
                ring_copy(way, 0, turn).start()

        @pl.when(jnp.logical_and(tick >= 1, tick < total + hops - 2))
        def _():
            for way in range(2):
                pl.semaphore_signal(
                    ring_free.at[way], inc=1, device_id=(t, origin[way]), device_id_type=MESH
                )

        @pl.when(jnp.logical_and(tick >= 1, tick < total + 1))
        def _():
            for tensor in range(tensors):
                raw_copy(tick - 1, tensor).wait()

        ahead = tick + SLOTS - 1

        @pl.when(jnp.logical_and(tick >= 1, ahead < total))
        def _():
            for step in range(1, tp_count):
                pl.semaphore_signal(
                    x_free.at[step - 1],
                    inc=1,
                    device_id=(lax.rem(t + tp_count - step, tp_count), g),
                    device_id_type=MESH,
                )

        @pl.when(ahead < total)
        def _():
            @pl.when(tick >= 1)
            def _():
                for step in range(1, tp_count):
                    x_copy(ahead - SLOTS, step).wait_send()

            choose(ahead)

            @pl.when(tick >= 1)
            def _():
                for step in range(1, tp_count):
                    pl.semaphore_wait(x_free.at[step - 1], 1)

            for step in range(1, tp_count):
                x_copy(ahead, step).start()

            @pl.when(ahead + 2 < total)
            def _():
                fetch_all(ahead + 2)

    @pl.loop(total - SLOTS, total)
    def _(index):
        for step in range(1, tp_count):
            x_copy(index, step).wait_send()

    for stage in range(hops):
        for way in range(2):
            for turn in range(2):
                ring_copy(way, stage, turn).wait_send()


def per_device(flat_shards, offsets, probes):
    tp_count = lax.axis_size("tp")
    grp_count = lax.axis_size("grp")
    layers, tensors, shard, total_width = flat_shards.shape
    pairs = layers * tensors
    rows = shard - PAD
    columns = total_width // tp_count
    probe_count = probes.shape[0]
    chunk = tensors * WIDTH
    share = probe_count // grp_count
    half = share // 2
    hops = grp_count - 1

    anywhere = pl.BlockSpec(memory_space=pl.ANY)
    inside = pl.BlockSpec(memory_space=pltpu.VMEM)
    dma = pltpu.SemaphoreType.DMA
    regular = pltpu.SemaphoreType.REGULAR
    return pl.pallas_call(
        functools.partial(exchange, tp_count, grp_count),
        out_shape=(
            jax.ShapeDtypeStruct((layers, tensors, tp_count * rows, columns), flat_shards.dtype),
            jax.ShapeDtypeStruct((layers, share, columns), jnp.bfloat16),
        ),
        in_specs=[anywhere, pl.BlockSpec(memory_space=pltpu.SMEM), inside],
        out_specs=(anywhere, inside),
        scratch_shapes=[
            pltpu.VMEM((2, tp_count, WIDTH // LANES, shard, tensors, LANES), flat_shards.dtype),
            pltpu.VMEM((pairs, rows, shard * tensors), flat_shards.dtype),
            pltpu.VMEM((SLOTS, tp_count - 1, rows, chunk), flat_shards.dtype),
            pltpu.VMEM((SLOTS, tp_count * rows, chunk), flat_shards.dtype),
            pltpu.VMEM((grp_count, probe_count, chunk), jnp.float32),
            pltpu.VMEM((2, hops, 2, half, chunk), jnp.float32),
            pltpu.VMEM((2, hops, 2, half, chunk), jnp.float32),
            dma((2, tp_count, WIDTH // LANES)),
            dma((tp_count - 1, SLOTS)),
            dma((tp_count - 1, SLOTS)),
            regular((tp_count - 1,)),
            dma((SLOTS, tensors)),
            dma((2, hops, 2)),
            dma((2, hops, 2)),
            regular((2,)),
        ],
        compiler_params=pltpu.CompilerParams(
            collective_id=0, has_side_effects=True, vmem_limit_bytes=60 * 1024 * 1024
        ),
    )(flat_shards.transpose(0, 2, 1, 3), offsets, probes)


def solution(mesh):
    placed = (P(None, None, ("grp", "tp"), None), P(), P(None, "grp"))
    return jax.shard_map(
        per_device,
        mesh=mesh,
        in_specs=placed,
        out_specs=(P(None, None, "grp", "tp"), P(None, "grp", "tp")),
        check_vma=False,
    )
```

```python
import functools

import jax
import jax.numpy as jnp
from jax import lax
from jax.experimental import pallas as pl
from jax.experimental.pallas import tpu as pltpu
from jax.sharding import PartitionSpec as P

PAD = 2
WIDTH = 128
LANES = 128
SLOTS = 6
MESH = pl.DeviceIdType.MESH


def ring_device(place, count):
    half = count // 2
    back = lax.div(place, half)
    return (1 - back) * 2 * place + back * (2 * (count - 1 - place) + 1)


def exchange(
    tp_count,
    grp_count,
    flat_ref,
    offsets_ref,
    probes_ref,
    raw_ref,
    check_ref,
    inbuf,
    chosen,
    sending,
    xbuf,
    partial,
    outgoing,
    incoming,
    in_sem,
    x_send,
    x_recv,
    x_free,
    raw_sem,
    ring_send,
    ring_recv,
    ring_free,
):
    t = lax.axis_index("tp")
    g = lax.axis_index("grp")
    odd = lax.rem(g, 2)
    place = (1 - odd) * lax.div(g, 2) + odd * (grp_count - 1 - lax.div(g, 2))
    after = ring_device(lax.rem(place + 1, grp_count), grp_count)
    before = ring_device(lax.rem(place + grp_count - 1, grp_count), grp_count)
    toward = (after, before)
    origin = (before, after)

    layers, shard, tensors, _ = flat_ref.shape
    rows = shard - PAD
    columns = raw_ref.shape[3]
    chunk = xbuf.shape[2]
    width = chunk // tensors
    per_layer = columns // width
    total = layers * per_layer
    share = probes_ref.shape[0] // grp_count
    half = share // 2
    hops = grp_count // 2
    firsts = (slice(0, half), slice(half, share))
    seconds = (slice(half, share), slice(0, half))

    def fetch(index, step, piece):
        layer, block = lax.div(index, per_layer), lax.rem(index, per_layer)
        turn = lax.rem(index, 2)
        partner = lax.rem(t + step, tp_count)
        start = pl.multiple_of(partner * columns + block * width + piece * LANES, LANES)
        return pltpu.make_async_copy(
            flat_ref.at[layer, :, :, pl.ds(start, LANES)],
            inbuf.at[turn, step, piece],
            in_sem.at[turn, step, piece],
        )

    def fetch_all(index):
        for step in range(tp_count):
            for piece in range(width // LANES):
                fetch(index, step, piece).start()

    def choose(index):
        layer = lax.div(index, per_layer)
        turn, slot = lax.rem(index, 2), lax.rem(index, SLOTS)
        for step in list(range(1, tp_count)) + [0]:
            pieces = []
            for piece in range(width // LANES):
                fetch(index, step, piece).wait()
                pieces.append(inbuf[turn, step, piece].reshape(shard * tensors, LANES))
            both = jnp.concatenate(pieces, axis=1)
            for tensor in range(tensors):
                picked = jnp.dot(
                    chosen[layer * tensors + tensor], both, preferred_element_type=jnp.float32
                ).astype(xbuf.dtype)
                where = slice(tensor * width, (tensor + 1) * width)
                if step == 0:
                    xbuf[slot, pl.ds(pl.multiple_of(t * rows, rows), rows), where] = picked
                else:
                    sending[slot, step - 1, :, where] = picked

    def x_copy(index, step):
        slot = lax.rem(index, SLOTS)
        return pltpu.make_async_remote_copy(
            src_ref=sending.at[slot, step - 1],
            dst_ref=xbuf.at[slot, pl.ds(pl.multiple_of(t * rows, rows), rows), :],
            send_sem=x_send.at[step - 1, slot],
            recv_sem=x_recv.at[step - 1, slot],
            device_id=(lax.rem(t + step, tp_count), g),
            device_id_type=MESH,
        )

    def x_arrival(index, step):
        slot = lax.rem(index, SLOTS)
        source = lax.rem(t + tp_count - step, tp_count)
        landing = xbuf.at[slot, pl.ds(pl.multiple_of(source * rows, rows), rows), :]
        return pltpu.make_async_remote_copy(
            src_ref=landing,
            dst_ref=landing,
            send_sem=x_send.at[step - 1, slot],
            recv_sem=x_recv.at[step - 1, slot],
            device_id=(source, g),
            device_id_type=MESH,
        )

    def raw_copy(index, tensor):
        layer, block = lax.div(index, per_layer), lax.rem(index, per_layer)
        slot = lax.rem(index, SLOTS)
        where = pl.ds(pl.multiple_of(block * width, width), width)
        return pltpu.make_async_copy(
            xbuf.at[slot, :, pl.ds(tensor * width, width)],
            raw_ref.at[layer, tensor, :, where],
            raw_sem.at[slot, tensor],
        )

    def ring_copy(way, stage, turn):
        part = firsts[way] if stage == 0 else slice(0, share)
        return pltpu.make_async_remote_copy(
            src_ref=outgoing.at[way, stage, turn, part],
            dst_ref=incoming.at[way, stage, turn, part],
            send_sem=ring_send.at[way, stage, turn],
            recv_sem=ring_recv.at[way, stage, turn],
            device_id=(t, toward[way]),
            device_id_type=MESH,
        )

    def own_rows(way, stage, part):
        away = hops - stage
        owner = lax.rem(place + (away if way == 0 else grp_count - away), grp_count)
        first = ring_device(owner, grp_count) * share + part.start
        size = part.stop - part.start
        return pl.ds(pl.multiple_of(first, half), size)

    barrier = pltpu.get_barrier_semaphore()
    for step in range(1, tp_count):
        pl.semaphore_signal(
            barrier, inc=1, device_id=(lax.rem(t + step, tp_count), g), device_id_type=MESH
        )
    for way in range(2):
        pl.semaphore_signal(barrier, inc=1, device_id=(t, toward[way]), device_id_type=MESH)
    fetch_all(0)
    fetch_all(1)
    at_row = lax.broadcasted_iota(jnp.int32, (rows, shard * tensors), 0)
    at_column = lax.broadcasted_iota(jnp.int32, (rows, shard * tensors), 1)
    for layer in range(layers):
        for tensor in range(tensors):
            wanted = (at_row + offsets_ref[layer, tensor]) * tensors + tensor
            chosen[layer * tensors + tensor] = jnp.where(at_column == wanted, 1.0, 0.0).astype(
                chosen.dtype
            )
    pl.semaphore_wait(barrier, tp_count - 1 + 2)

    @pl.loop(0, SLOTS - 1)
    def _(index):
        choose(index)
        for step in range(1, tp_count):
            x_copy(index, step).start()
        fetch_all(index + 2)

    @pl.loop(0, total + hops)
    def _(tick):
        turn = lax.rem(tick, 2)
        last_turn = 1 - turn

        @pl.when(jnp.logical_and(tick >= 2, tick < total + hops - 1))
        def _():
            for way in range(2):
                pl.semaphore_wait(ring_free.at[way], 1)

        for stage in range(hops, 0, -1):
            index = tick - stage

            @pl.when(jnp.logical_and(index >= 0, index < total))
            def _():
                place_of = lax.rem(index, hops)
                if stage < hops:

                    @pl.when(index >= 2)
                    def _():
                        for way in range(2):
                            ring_copy(way, stage, turn).wait_send()

                    for way in range(2):
                        ring_copy(way, stage - 1, last_turn).wait_recv()
                        adds = (firsts[way],) if stage == 1 else firsts
                        for part in adds:
                            outgoing[way, stage, turn, part] = (
                                incoming[way, stage - 1, last_turn, part]
                                + partial[place_of, own_rows(way, stage, part), :]
                            )
                        if stage == 1:
                            part = seconds[way]
                            outgoing[way, stage, turn, part] = partial[
                                place_of, own_rows(way, stage, part), :
                            ]
                        ring_copy(way, stage, turn).start()
                else:
                    layer, block = lax.div(index, per_layer), lax.rem(index, per_layer)
                    for way in range(2):
                        ring_copy(way, stage - 1, last_turn).wait_recv()
                    sums = (
                        partial[place_of, own_rows(0, stage, slice(0, share)), :]
                        + incoming[0, stage - 1, last_turn]
                        + incoming[1, stage - 1, last_turn]
                    )
                    gate, up = sums[:, :width], sums[:, width:]
                    hidden = gate / (1.0 + jnp.exp(-gate)) * up
                    where = pl.ds(pl.multiple_of(block * width, width), width)
                    check_ref[layer, :, where] = hidden.astype(check_ref.dtype)

        @pl.when(tick < total)
        def _():
            slot = lax.rem(tick, SLOTS)
            kept = lax.rem(tick, hops)
            for step in range(1, tp_count):
                x_arrival(tick, step).wait_recv()
            for tensor in range(tensors):
                raw_copy(tick, tensor).start()
            partial[kept] = jnp.dot(
                probes_ref[...], xbuf[slot], preferred_element_type=jnp.float32
            )

            @pl.when(tick >= 2)
            def _():
                for way in range(2):
                    ring_copy(way, 0, turn).wait_send()

            for way in range(2):
                part = firsts[way]
                outgoing[way, 0, turn, part] = partial[kept, own_rows(way, 0, part), :]
                ring_copy(way, 0, turn).start()

        @pl.when(jnp.logical_and(tick >= 1, tick < total + hops - 2))
        def _():
            for way in range(2):
                pl.semaphore_signal(
                    ring_free.at[way], inc=1, device_id=(t, origin[way]), device_id_type=MESH
                )

        @pl.when(jnp.logical_and(tick >= 1, tick < total + 1))
        def _():
            for tensor in range(tensors):
                raw_copy(tick - 1, tensor).wait()

        ahead = tick + SLOTS - 1

        @pl.when(jnp.logical_and(tick >= 1, ahead < total))
        def _():
            for step in range(1, tp_count):
                pl.semaphore_signal(
                    x_free.at[step - 1],
                    inc=1,
                    device_id=(lax.rem(t + tp_count - step, tp_count), g),
                    device_id_type=MESH,
                )

        @pl.when(ahead < total)
        def _():
            @pl.when(tick >= 1)
            def _():
                for step in range(1, tp_count):
                    x_copy(ahead - SLOTS, step).wait_send()

            choose(ahead)

            @pl.when(tick >= 1)
            def _():
                for step in range(1, tp_count):
                    pl.semaphore_wait(x_free.at[step - 1], 1)

            for step in range(1, tp_count):
                x_copy(ahead, step).start()

            @pl.when(ahead + 2 < total)
            def _():
                fetch_all(ahead + 2)

    @pl.loop(total - SLOTS, total)
    def _(index):
        for step in range(1, tp_count):
            x_copy(index, step).wait_send()

    for stage in range(hops):
        for way in range(2):
            for turn in range(2):
                ring_copy(way, stage, turn).wait_send()


def per_device(flat_shards, offsets, probes):
    tp_count = lax.axis_size("tp")
    grp_count = lax.axis_size("grp")
    layers, tensors, shard, total_width = flat_shards.shape
    pairs = layers * tensors
    rows = shard - PAD
    columns = total_width // tp_count
    probe_count = probes.shape[0]
    chunk = tensors * WIDTH
    share = probe_count // grp_count
    hops = grp_count // 2

    anywhere = pl.BlockSpec(memory_space=pl.ANY)
    inside = pl.BlockSpec(memory_space=pltpu.VMEM)
    dma = pltpu.SemaphoreType.DMA
    regular = pltpu.SemaphoreType.REGULAR
    return pl.pallas_call(
        functools.partial(exchange, tp_count, grp_count),
        out_shape=(
            jax.ShapeDtypeStruct((layers, tensors, tp_count * rows, columns), flat_shards.dtype),
            jax.ShapeDtypeStruct((layers, share, columns), jnp.bfloat16),
        ),
        in_specs=[anywhere, pl.BlockSpec(memory_space=pltpu.SMEM), inside],
        out_specs=(anywhere, inside),
        scratch_shapes=[
            pltpu.VMEM((2, tp_count, WIDTH // LANES, shard, tensors, LANES), flat_shards.dtype),
            pltpu.VMEM((pairs, rows, shard * tensors), flat_shards.dtype),
            pltpu.VMEM((SLOTS, tp_count - 1, rows, chunk), flat_shards.dtype),
            pltpu.VMEM((SLOTS, tp_count * rows, chunk), flat_shards.dtype),
            pltpu.VMEM((hops, probe_count, chunk), jnp.float32),
            pltpu.VMEM((2, hops, 2, share, chunk), jnp.float32),
            pltpu.VMEM((2, hops, 2, share, chunk), jnp.float32),
            dma((2, tp_count, WIDTH // LANES)),
            dma((tp_count - 1, SLOTS)),
            dma((tp_count - 1, SLOTS)),
            regular((tp_count - 1,)),
            dma((SLOTS, tensors)),
            dma((2, hops, 2)),
            dma((2, hops, 2)),
            regular((2,)),
        ],
        compiler_params=pltpu.CompilerParams(
            collective_id=0, has_side_effects=True, vmem_limit_bytes=60 * 1024 * 1024
        ),
    )(flat_shards.transpose(0, 2, 1, 3), offsets, probes)


def solution(mesh):
    placed = (P(None, None, ("grp", "tp"), None), P(), P(None, "grp"))
    return jax.shard_map(
        per_device,
        mesh=mesh,
        in_specs=placed,
        out_specs=(P(None, None, "grp", "tp"), P(None, "grp", "tp")),
        check_vma=False,
    )
```
